32 devices in a mesh: ep: 8 (over z, y), fsdp: 4 (over x, core).
Axes of the slice: x: 2, y: 2, z: 4, core: 2. Of those that a mesh axis runs over, the one named last changes fastest.
Arguments:
- train_gate: float32 [64, 2048, 1024], P('ep', 'fsdp'), may hold values from -0.1875 to 0.1875
- other_gate: float32 [64, 2048, 1024], P('ep', 'fsdp'), may hold values from -0.125 to 0.125
- train_up: float32 [64, 2048, 1024], P('ep', 'fsdp'), may hold values from -0.1875 to 0.1875
- other_up: float32 [64, 2048, 1024], P('ep', 'fsdp'), may hold values from -0.125 to 0.125
- mix_share: float32 [64], P('ep'), may hold values from 0.2 to 0.8
- router_weight: float32 [2048, 64], P('fsdp', 'ep'), may hold values from -0.125 to 0.125
- router_gain: float32 [2048], P('fsdp'), may hold values from 0.25 to 1.75
Outputs:
- ready_gate: bfloat16 [64, 2048, 1024], P('ep')
- ready_up: bfloat16 [64, 2048, 1024], P('ep')
- scale_gate: float32 [64, 1024], P('ep')
- scale_up: float32 [64, 1024], P('ep')
- serve_router: bfloat16 [2048, 64], replicated
The draws below stay inside these ranges and needn't reach their ends.
All inputs are finite; a program needn't handle non-finite values. Where the reference program divides by a largest or mean magnitude, that divisor is 1e-20 or more.
Results may differ from the reference program's by a relative error of at most 0.001.
Values may be sent and summed in bfloat16 or wider, within the bound.
A program may use at most 256 MiB of HBM per device.

```python
import jax
import jax.numpy as jnp

EXPERTS = 64
D_MODEL = 2048
D_EXPERT = 1024


def with_spikes(drawn, stream_key, source, target, shards_of, factor):
    owner, partner = [(jnp.arange(drawn.shape[dim]) // (drawn.shape[dim] // shards_of)).reshape([-1 if axis == dim else 1 for axis in range(drawn.ndim)]) for dim in (source, target)]
    chosen = jax.random.permutation(stream_key, shards_of)[partner]
    strong = (owner == chosen) | (owner == (partner + shards_of // 2) % shards_of)
    return jnp.where(strong, factor * drawn, drawn)


def steps_of(key, dims, split, least, top_value):
    def one(position, shards_of):
        steps = jax.random.uniform(jax.random.fold_in(jax.random.fold_in(key, 6), position), (shards_of,), jnp.float32, least / len(split), top_value / len(split))
        return jnp.repeat(jnp.exp(steps), dims[position] // shards_of).reshape((-1,) + (1,) * (len(dims) - position - 1))

    gain = one(*split[0])
    for cut in split[1:]:
        gain = gain * one(*cut)
    return gain


def bell_draw(key, shape, spread, bound, pieces=(), dtype=jnp.bfloat16):
    result = jax.random.normal(key, shape, jnp.float32) * spread
    if len(pieces) > 0:
        result = steps_of(key, shape, pieces, -0.22, 0.18) * result
    return jnp.clip(result, min=-bound, max=bound).astype(dtype)


def bell_draw_with(stream_key, dims, width, reach, cuts, heavy, kind=jnp.bfloat16):
    drawn = width * jax.random.normal(stream_key, dims, jnp.float32)
    if cuts:
        drawn = drawn * steps_of(stream_key, dims, cuts, -0.22, 0.18)
    return jnp.clip(with_spikes(drawn, jax.random.fold_in(stream_key, 3), *heavy), -reach, reach).astype(kind)


def setup_inputs(seed: int = 0) -> dict:
    arg_keys = jax.random.split(jax.random.key(seed), 8)
    train_gate = bell_draw_with(arg_keys[0], (EXPERTS, D_MODEL, D_EXPERT), D_MODEL ** -0.5, 0.1875, ((0, 8), (1, 4)), (1, 2, 4, 2.0), jnp.float32)
    other_gate = bell_draw(arg_keys[1], (EXPERTS, D_MODEL, D_EXPERT), D_MODEL ** -0.5, 0.125, ((0, 8), (1, 4)), jnp.float32)
    train_up = bell_draw_with(arg_keys[2], (EXPERTS, D_MODEL, D_EXPERT), D_MODEL ** -0.5, 0.1875, ((0, 8), (1, 4)), (1, 2, 4, 2.0), jnp.float32)
    other_up = bell_draw(arg_keys[3], (EXPERTS, D_MODEL, D_EXPERT), D_MODEL ** -0.5, 0.125, ((0, 8), (1, 4)), jnp.float32)
    mix_share = jnp.clip(0.2 + 0.6 * jax.random.uniform(arg_keys[4], (EXPERTS,), jnp.float32) ** steps_of(arg_keys[4], (EXPERTS,), ((0, 8),), -0.2, 0.2), 0.2, 0.8)
    router_weight = bell_draw(arg_keys[5], (D_MODEL, EXPERTS), D_MODEL ** -0.5, 0.125, ((0, 4), (1, 8)), jnp.float32)
    router_gain = jnp.clip(1.0 + 0.15 * jax.random.normal(arg_keys[6], (D_MODEL,), jnp.float32), 0.25, 1.75)
    return dict(train_gate=train_gate, other_gate=other_gate, train_up=train_up, other_up=other_up, mix_share=mix_share, router_weight=router_weight, router_gain=router_gain)


def reference(train_gate, other_gate, train_up, other_up, mix_share, router_weight, router_gain):
    latest_gate = mix_share[:, None, None] * train_gate + (1.0 - mix_share[:, None, None]) * other_gate
    latest_up = mix_share[:, None, None] * train_up + (1.0 - mix_share[:, None, None]) * other_up
    scale_gate = jnp.max(jnp.abs(latest_gate), axis=1)
    ready_gate = (latest_gate / jnp.expand_dims(scale_gate, 1)).astype(jnp.bfloat16)
    scale_up = jnp.max(jnp.abs(latest_up), axis=1)
    ready_up = (latest_up / jnp.expand_dims(scale_up, 1)).astype(jnp.bfloat16)
    serve_router = (router_weight * router_gain[:, None]).astype(jnp.bfloat16)
    return ready_gate, ready_up, scale_gate, scale_up, serve_router
```

```python
import jax
import jax.numpy as jnp
from jax import lax
from jax.experimental import pallas as pl
from jax.sharding import PartitionSpec as P


def swap(value, axis, size, bit):
    return lax.ppermute(value, axis, [(i, i ^ bit) for i in range(size)])


def blank(shape):
    return pl.pallas_call(
        lambda out: None,
        out_shape=jax.ShapeDtypeStruct(shape, jnp.bfloat16),
        out_specs=pl.BlockSpec(memory_space=pl.ANY),
    )()


def bits_of(size):
    assert size & (size - 1) == 0
    return [1 << b for b in range(size.bit_length() - 1)]


def solution(mesh):
    fsdp, ep = mesh.shape["fsdp"], mesh.shape["ep"]
    rows_bits, ep_bits = bits_of(fsdp), bits_of(ep)

    def largest(value):
        others = [swap(value, "fsdp", fsdp, d) for d in range(1, fsdp)]
        for other in others:
            value = jnp.maximum(value, other)
        return value

    def double(value, axis, size, bit, done):
        other = swap(value, axis, size, bit)
        upper = (lax.axis_index(axis) & bit) != 0
        return jnp.stack([jnp.where(upper, other, value), jnp.where(upper, value, other)], axis=done)

    def per_device(train_gate, other_gate, train_up, other_up, mix_share, router_weight, router_gain):
        experts, depth, width = train_gate.shape
        me = lax.axis_index("fsdp")
        pairs = ((train_gate, other_gate), (train_up, other_up))
        chunks = [(e, w) for e in range(experts) for w in range(2)]

        def mixed(chunk, share):
            e, w = chunk
            train, other = pairs[w]
            return share[e] * train[e] + (1.0 - share[e]) * other[e]

        def tops(group, share):
            return jnp.stack([jnp.max(jnp.abs(mixed(c, share)), axis=0) for c in group])

        def narrow(chunk, share, scale):
            return (mixed(chunk, share) / scale[None]).astype(jnp.bfloat16)

        total = len(chunks)
        cuts = [min(c, total) for c in (0, 2, 7)] + [total]
        groups = [chunks[i:j] for i, j in zip(cuts, cuts[1:]) if j > i]
        share, scales, owns, crossed = mix_share, [], [], []
        top_bit, low_bits = rows_bits[-1], rows_bits[:-1][::-1]

        def send(n):
            crossed.append(swap(owns[n], "fsdp", fsdp, top_bit))

        local = tops(groups[0], share)
        share, local = lax.optimization_barrier((share, local))
        scale = largest(local)
        for g, group in enumerate(groups):
            scales.append(scale)
            for i, c in enumerate(group):
                n = len(owns)
                if n >= 4:
                    share, crossed[n - 4] = lax.optimization_barrier((share, crossed[n - 4]))
                own = narrow(c, share, scale[i])
                share, own = lax.optimization_barrier((share, own))
                if n >= 2:
                    crossed[n - 2], own = lax.optimization_barrier((crossed[n - 2], own))
                owns.append(own)
                send(n)
                if i == 0 and g + 1 < len(groups):
                    local = tops(groups[g + 1], share)
                    share, local = lax.optimization_barrier((share, local))
                    ahead = largest(local)
            if g + 1 < len(groups):
                scale = ahead

        def across(held):
            for bit in low_bits:
                held = held + [(place ^ bit, swap(piece, "fsdp", fsdp, bit)) for place, piece in held]
            return held

        def put(out, e, held):
            for place, piece in held:
                out = lax.dynamic_update_slice(out, piece[None, None], (e, place, 0, 0))
            return out

        outs = [blank((experts, fsdp, depth, width)) for _ in range(2)]
        for n in range(total):
            e, w = chunks[n]
            outs[w] = put(outs[w], e, across([(me, owns[n])]))
            outs[w] = put(outs[w], e, across([(me ^ top_bit, crossed[n])]))
        ready = [o.reshape(experts, fsdp * depth, width) for o in outs]
        scales = jnp.concatenate(scales, axis=0).reshape(experts, 2, width)

        whole = (router_weight * router_gain[:, None]).astype(jnp.bfloat16).T
        wide = whole.shape
        for done, bit in enumerate(rows_bits[::-1]):
            whole = double(whole, "fsdp", fsdp, bit, done)
            if done == 0:
                whole, _ = lax.optimization_barrier((whole, crossed[total // 2]))
        whole = jnp.moveaxis(whole.reshape(fsdp, *wide), 0, 1).reshape(wide[0], fsdp * wide[1])
        for done, bit in enumerate(ep_bits[::-1]):
            whole = double(whole, "ep", ep, bit, done)
        whole = whole.reshape(ep * wide[0], fsdp * wide[1])
        return ready[0], ready[1], scales[:, 0], scales[:, 1], whole.T

    placed = (
        P("ep", "fsdp", None),
        P("ep", "fsdp", None),
        P("ep", "fsdp", None),
        P("ep", "fsdp", None),
        P("ep"),
        P("fsdp", "ep"),
        P("fsdp"),
    )
    return jax.shard_map(
        per_device,
        mesh=mesh,
        in_specs=placed,
        out_specs=(P("ep", None, None), P("ep", None, None), P("ep", None), P("ep", None), P()),
        check_vma=False,
    )
```
